128 devices in a mesh: gx: 4 (over x_lo, core), gy: 4 (over z), gz: 8 (over x_hi, y).
Axes of the slice: x: 4 (x_hi: 2, x_lo: 2; x = x_hi * 2 + x_lo), y: 4, z: 4, core: 2. Of those that a mesh axis runs over, the one named last changes fastest.
Arguments:
- fields: float32 [11, 500, 32, 1024], P(None, 'gx', 'gy', 'gz'), may hold values from -6 to 6
- var_scale: float32 [11], replicated, may hold values from 0.3 to 3
- start_basis: float32 [500, 64], replicated, may hold values from -6 to 6
Outputs:
- factor: float32 [500, 64], replicated
- core: float32 [64, 11, 32, 1024], P('gx', None, 'gy', 'gz')
The draws below stay inside these ranges and needn't reach their ends.
All inputs are finite; a program needn't handle non-finite values.
Results may differ from the reference program's by a relative error of at most 0.0002.
Values sent between devices are 32-bit elements; how exact they have to be, the bound alone decides.
A program may use at most 128 MiB of HBM per device.

```python
import math
import jax
import jax.numpy as jnp
from jax import lax

V = 11
N1 = 500
RANK = 64
ITERS = 3
N2 = 32
N3 = 1024


def steps_of(stream_key, dims, shards, low, largest):
    def one(dim, shards_of):
        heights = jax.random.uniform(jax.random.fold_in(jax.random.fold_in(stream_key, 6), dim), (shards_of,), jnp.float32, low / len(shards), largest / len(shards))
        return jnp.repeat(jnp.exp(heights), dims[dim] // shards_of).reshape((-1,) + (1,) * (len(dims) - dim - 1))

    level = one(*shards[0])
    for cut in shards[1:]:
        level = level * one(*cut)
    return level


def centred(key, shape, width, limit, split=(), dtype=jnp.bfloat16):
    array = jax.random.normal(key, shape, jnp.float32) * width
    if len(split) > 0:
        array = steps_of(key, shape, split, -0.22, 0.18) * array
    return jnp.clip(array, min=-limit, max=limit).astype(dtype)


def setup_inputs(seed: int = 0) -> dict:
    splits = jax.random.split(jax.random.key(seed), 4)
    fields = centred(splits[0], (V, N1, N2, N3), 1.0, 6.0, ((1, 4), (2, 4), (3, 8)), jnp.float32)
    var_scale = jnp.clip(jnp.exp(jax.random.uniform(splits[1], (V,), jnp.float32, math.log(0.3), math.log(3.0))), 0.3, 3.0)
    start_basis = centred(splits[2], (N1, RANK), 1.0, 6.0, (), jnp.float32)
    return dict(fields=fields, var_scale=var_scale, start_basis=start_basis)


def orthonormal(block):
    small = jnp.dot(block.T, block, precision=lax.Precision.HIGHEST)
    lower = jnp.linalg.cholesky(small)
    return jax.scipy.linalg.solve_triangular(lower, block.T, lower=True).T

def reference(fields, var_scale, start_basis):
    scaled = fields * var_scale[:, None, None, None]
    gram = lax.dot_general(scaled, scaled, (((0, 2, 3), (0, 2, 3)), ((), ())), precision=lax.Precision.HIGHEST)
    basis = start_basis
    for step in range(ITERS):
        basis = orthonormal(jnp.dot(gram, basis, precision=lax.Precision.HIGHEST))
    core = lax.dot_general(basis, scaled, (((0,), (1,)), ((), ())), precision=lax.Precision.HIGHEST)
    return (basis, core)
```

```python
import functools

import jax
import jax.numpy as jnp
from jax import lax
from jax.experimental import pallas as pl
from jax.experimental.pallas import tpu as pltpu
from jax.sharding import PartitionSpec as P

ITERS = 3
MESH = pl.DeviceIdType.MESH
NN = (((1,), (0,)), ((), ()))
NT = (((1,), (1,)), ((), ()))
F32 = jnp.float32
BF16 = jnp.bfloat16
HI = lax.Precision.HIGHEST


def split(x):
    hi = x.astype(BF16)
    return hi, (x - hi.astype(F32)).astype(BF16)


def dot(a, b, dims):
    return lax.dot_general(a, b, dims, preferred_element_type=F32)


def dot3(ah, al, bh, bl, dims):
    return dot(ah, bh, dims) + (dot(ah, bl, dims) + dot(al, bh, dims))


def column(block, j):
    return block.reshape(512, 128)[pl.ds(j, 128, stride=4), :]


def eliminate(m):
    tiles = [m[8 * t : 8 * t + 8, :] for t in range(8)]
    sub = lax.broadcasted_iota(jnp.int32, (8, 128), 0)
    for q in range(8):
        cols = [
            {t: jnp.broadcast_to(tiles[t][:, 8 * q + k : 8 * q + k + 1], (8, 128)) for t in range(q, 8)}
            for k in range(8)
        ]
        pivots = jnp.ones((8, 128), F32)
        for k in range(8):
            p = jnp.broadcast_to(cols[k][q][k : k + 1, :], (8, 128))
            rp = 1.0 / p
            row = jnp.broadcast_to(tiles[q][k : k + 1, :], (8, 128))
            across = {l: jnp.broadcast_to(cols[l][q][k : k + 1, :], (8, 128)) for l in range(k + 1, 8)}
            for t in range(q, 8):
                f = cols[k][t] * rp
                if t == q:
                    f = jnp.where(sub > k, f, 0.0)
                tiles[t] = tiles[t] - f * row
                for l in range(k + 1, 8):
                    cols[l][t] = cols[l][t] - f * across[l]
            pivots = jnp.where(sub == k, p, pivots)
        r = lax.rsqrt(pivots)
        r = r * (1.5 - 0.5 * (pivots * r) * r)
        tiles[q] = tiles[q] * r
    return jnp.concatenate(tiles, axis=0)


def kernel(
    nv, nz, ny, scale_ref, x_ref, start_ref,
    factor_ref, core_ref,
    xo, xd, xx, xf, Xh, Xl, Yh, Yl,
    acc_own, acc_ab,
    zb_o, b1_o, yb_o, b2_o, xb_o, zb_a, b1_a, yb_a, b2_a, xb_a,
    gd, gx_, gh, gl, bt, fh, fl, psend, precv,
    s_loc, s_d2d, s_x, s_fw, s_ro, s_ra, s_g, s_c,
):
    me = lax.axis_index("gx")
    z = lax.axis_index("gy")
    hy = lax.axis_index("gz")
    h = me // 2
    c = lax.rem(me, 2)
    o = 1 - h
    xh = hy // ny
    y = lax.rem(hy, ny)
    rz = 128 // nz
    ry = rz // ny

    def dev(gx=me, gy=z, xhi=xh, yy=y):
        return {"gx": gx, "gy": gy, "gz": xhi * ny + yy}

    mate = dev(gx=2 * h + (1 - c))
    across = dev(gx=2 * o + c)
    zs = [dev(gy=lax.rem(z + d, nz)) for d in range(1, nz)]
    ys = [dev(yy=lax.rem(y + d, ny)) for d in range(1, ny)]
    x_hi = dev(xhi=1 - xh)
    x_all = [x_hi, across, dev(gx=2 * o + c, xhi=1 - xh)]

    def rcopy(src, dst, sems, at, to):
        return pltpu.make_async_remote_copy(
            src_ref=src, dst_ref=dst, send_sem=sems.at[(0,) + at], recv_sem=sems.at[(1,) + at],
            device_id=to, device_id_type=MESH,
        )

    def local(v, half):
        return pltpu.make_async_copy(x_ref.at[v, :, half], xo.at[v, half, 0:125], s_loc.at[v, half])

    def c_d2d(v):
        return rcopy(xo.at[v, :, 0:125], xd.at[v, :, 0:125], s_d2d, (v,), mate)

    def c_x(v):
        return rcopy(xo.at[v, o, 0:125], xx.at[v, 0:125], s_x, (v,), across)

    def c_fw(v):
        return rcopy(xx.at[v, 0:125], xf.at[v, 0:125], s_fw, (v,), mate)

    for v in range(nv):
        local(v, o).start()
        local(v, h).start()

    barrier = pltpu.get_barrier_semaphore()
    greet = [mate] + zs + ys + x_all
    for d in greet:
        pl.semaphore_signal(barrier, inc=1, device_id=d, device_id_type=MESH)
    zero = jnp.zeros((3, 4, 128), F32)
    for v in range(nv):
        for half in range(2):
            xo[v, half, 125:128] = zero
            xd[v, half, 125:128] = zero
        xx[v, 125:128] = zero
        xf[v, 125:128] = zero
    pl.semaphore_wait(barrier, len(greet))

    @pl.loop(0, nv)
    def _(v):
        local(v, o).wait()
        c_x(v).start()
        local(v, h).wait()
        c_d2d(v).start()

    acc_own[...] = jnp.zeros_like(acc_own)
    acc_ab[...] = jnp.zeros_like(acc_ab)
    zrow = jnp.zeros((3, 64), F32)
    for g in range(4):
        part = jnp.concatenate([start_ref[125 * g : 125 * g + 125, :], zrow], axis=0)
        bt[:, 128 * g : 128 * g + 128] = part.T

    def convert(block, s, dh, dl):
        for j in range(4):
            hi, lo = split(column(block, j) * s)
            dh[:, 128 * j : 128 * j + 128] = hi
            dl[:, 128 * j : 128 * j + 128] = lo

    def rows(g, n=128):
        return pl.ds(pl.multiple_of(g * 128, 128), n)

    @pl.loop(0, nv)
    def _(v):
        s = scale_ref[v]
        convert(xo.at[v, h], s, Xh.at[v, rows(me)], Xl.at[v, rows(me)])
        convert(xo.at[v, o], s, Yh.at[rows(c)], Yl.at[rows(c)])
        c_d2d(v).wait_recv()
        m2 = 2 * h + (1 - c)
        convert(xd.at[v, h], s, Xh.at[v, rows(m2)], Xl.at[v, rows(m2)])
        convert(xd.at[v, o], s, Yh.at[rows(1 - c)], Yl.at[rows(1 - c)])
        chip = pl.ds(pl.multiple_of(h * 256, 256), 256)
        acc_own[...] += dot3(
            Xh[v, rows(me), :], Xl[v, rows(me), :], Xh[v, chip, :], Xl[v, chip, :], NT
        ) + dot3(Yh[rows(c), :], Yl[rows(c), :], Yh[...], Yl[...], NT)

    class Reduce:
        def __init__(self, acc, zb, b1, yb, b2, xb, out, sems, partners, slot, slots):
            self.acc, self.zb, self.b1, self.yb, self.b2, self.xb = acc, zb, b1, yb, b2, xb
            self.out, self.sems, self.partners, self.slot, self.slots = out, sems, partners, slot, slots

        def at(self, n, start):
            return pl.ds(pl.multiple_of(start, ry), n)

        def zc(self, d):
            to = lax.rem(z + d, nz)
            return rcopy(self.acc.at[self.at(rz, to * rz)], self.zb.at[d - 1], self.sems, (0, d - 1), zs[d - 1])

        def yc(self, d):
            to = lax.rem(y + d, ny)
            return rcopy(self.b1.at[self.at(ry, to * ry)], self.yb.at[d - 1], self.sems, (1, d - 1), ys[d - 1])

        def xc(self, k):
            return rcopy(self.b2, self.xb.at[self.slot], self.sems, (2, k), self.partners[k])

        def yg(self, d):
            here = self.out.at[self.at(ry, c * 128 + z * rz + y * ry)]
            return rcopy(here, here, self.sems, (3, d - 1), ys[d - 1])

        def zg(self, d):
            here = self.out.at[self.at(rz, c * 128 + z * rz)]
            return rcopy(here, here, self.sems, (4, d - 1), zs[d - 1])

        def s0(self):
            for d in range(1, nz):
                self.zc(d).start()

        def s1(self):
            for d in range(1, nz):
                self.zc(d).wait_recv()
            t = self.acc[self.at(rz, z * rz), :]
            for d in range(1, nz):
                t = t + self.zb[d - 1]
            self.b1[...] = t
            for d in range(1, ny):
                self.yc(d).start()

        def s2(self):
            for d in range(1, ny):
                self.yc(d).wait_recv()
            t = self.b1[self.at(ry, y * ry), :]
            for d in range(1, ny):
                t = t + self.yb[d - 1]
            self.b2[...] = t
            for k in range(len(self.partners)):
                self.xc(k).start()
            self.xb[self.slot] = t

        def s3(self):
            for k in range(len(self.partners)):
                self.xc(k).wait_recv()
            t = self.xb[0]
            for k in range(1, self.slots):
                t = t + self.xb[k]
            self.out[self.at(ry, c * 128 + z * rz + y * ry), :] = t
            for d in range(1, ny):
                self.yg(d).start()

        def s4(self):
            for d in range(1, ny):
                self.yg(d).wait_recv()
            for d in range(1, nz):
                self.zg(d).start()

        def s5(self):
            for d in range(1, nz):
                self.zg(d).wait_recv()

        def finish(self):
            for d in range(1, nz):
                self.zc(d).wait_send()
                self.zg(d).wait_send()
            for d in range(1, ny):
                self.yc(d).wait_send()
                self.yg(d).wait_send()
            for k in range(len(self.partners)):
                self.xc(k).wait_send()

    own = Reduce(acc_own, zb_o, b1_o, yb_o, b2_o, xb_o, gd.at[h], s_ro, [x_hi], xh, 2)
    ab = Reduce(acc_ab, zb_a, b1_a, yb_a, b2_a, xb_a, gx_, s_ra, x_all, xh * 2 + h, 4)

    own.s0()
    steps = {1: own.s1, 3: own.s2, 5: own.s3, 7: own.s4, 9: own.s5}

    @pl.loop(0, nv)
    def _(v):
        s = scale_ref[v]
        c_x(v).wait_recv()
        c_fw(v).start()
        g2 = 2 * o + c
        convert(xx.at[v], s, Xh.at[v, rows(g2)], Xl.at[v, rows(g2)])
        for k, f in steps.items():
            pl.when(v == k * nv // 11)(f)
        c_fw(v).wait_recv()
        g3 = 2 * o + (1 - c)
        convert(xf.at[v], s, Xh.at[v, rows(g3)], Xl.at[v, rows(g3)])
        acc_ab[...] += dot3(
            Xh[v, rows(c), :], Xl[v, rows(c), :], Xh[v, 256:512, :], Xl[v, 256:512, :], NT
        )

    mine = pl.ds(pl.multiple_of(c * 128, 128), 128)
    g_d2d = rcopy(gd.at[h, mine], gd.at[h, mine], s_g, (0,), mate)
    g_x = rcopy(gd.at[h, mine], gd.at[h, mine], s_g, (1,), across)
    g_got = rcopy(gd.at[o, mine], gd.at[o, mine], s_g, (1,), across)
    g_fw = rcopy(gd.at[o, mine], gd.at[o, mine], s_g, (2,), mate)
    g_ab = rcopy(gx_.at[mine], gx_.at[mine], s_g, (3,), mate)
    ab.s0()
    g_x.start()
    g_d2d.start()
    ab.s1()
    ab.s2()
    g_got.wait_recv()
    g_fw.start()
    ab.s3()
    g_d2d.wait_recv()
    g_fw.wait_recv()
    ab.s4()
    gh[0:256], gl[0:256] = split(gd[0])
    gh[256:512], gl[256:512] = split(gd[1])
    ab.s5()
    g_ab.start()
    g_ab.wait_recv()
    gh[512:768], gl[512:768] = split(gx_[...])

    pad = jnp.zeros((64, 512), F32)
    rr = lax.broadcasted_iota(jnp.int32, (64, 128), 0)
    cc = lax.broadcasted_iota(jnp.int32, (64, 128), 1)
    eye = jnp.where(cc == rr + 64, 1.0, 0.0).astype(F32)

    @pl.loop(0, ITERS)
    def _(step):
        bh, bl = split(bt[...])
        d0 = gh[0:256, :], gl[0:256, :]
        d1 = gh[256:512, :], gl[256:512, :]
        ax = gh[512:768, :], gl[512:768, :]
        ba = bh[:, 0:256], bl[:, 0:256]
        bb = bh[:, 256:512], bl[:, 256:512]
        left = dot3(*ba, *d0, NN) + dot3(*bb, *ax, NT)
        right = dot3(*ba, *ax, NN) + dot3(*bb, *d1, NN)
        block = jnp.concatenate([left, right], axis=1)
        small = lax.dot_general(
            block, jnp.concatenate([block, pad], axis=0), NT, precision=HI, preferred_element_type=F32
        )
        w = eliminate(small + eye)
        w = jnp.where(cc >= 64, w, 0.0)
        bt[...] = lax.dot_general(
            w, jnp.concatenate([pad, block], axis=0), NN, precision=HI, preferred_element_type=F32
        )

    hi, lo = split(bt[...])
    fh[...] = hi
    fl[...] = lo

    def ranks(g):
        return pl.ds(pl.multiple_of(g * 16, 16), 16)

    def c_core(v):
        return rcopy(psend.at[v], precv.at[v], s_c, (v,), across)

    ours, theirs = ranks(me), ranks(2 * o + c)

    @pl.loop(0, nv)
    def _(v):
        ah = jnp.concatenate([fh[theirs, :], fh[ours, :]], axis=0)
        al = jnp.concatenate([fl[theirs, :], fl[ours, :]], axis=0)
        res = dot3(ah, al, Xh[v], Xl[v], NN)
        psend[v] = res[0:16]
        c_core(v).start()
        for j in range(4):
            core_ref[pl.ds(v * 8 + 4 * h + j, 16, stride=8 * nv), :] = res[16:32, 128 * j : 128 * j + 128]

    for g in range(4):
        factor_ref[125 * g : 125 * g + 125, :] = bt[:, 128 * g : 128 * g + 128].T[0:125, :]

    @pl.loop(0, nv)
    def _(v):
        c_core(v).wait_recv()
        got = precv[v]
        for j in range(4):
            core_ref[pl.ds(v * 8 + 4 * o + j, 16, stride=8 * nv), :] = got[:, 128 * j : 128 * j + 128]

    @pl.loop(0, nv)
    def _(v):
        c_x(v).wait_send()
        c_d2d(v).wait_send()
        c_fw(v).wait_send()
        c_core(v).wait_send()

    own.finish()
    ab.finish()
    for g in (g_d2d, g_x, g_fw, g_ab):
        g.wait_send()


def per_device(nz, ny, fields, var_scale, start_basis):
    nv = fields.shape[0]
    x = fields.reshape(nv, 125, 2, 4, 128)
    rz = 128 // nz
    ry = rz // ny
    block = (128, 4, 128)
    reduce_bufs = lambda slots: [
        pltpu.VMEM((max(nz - 1, 1), rz, 256), F32),
        pltpu.VMEM((rz, 256), F32),
        pltpu.VMEM((max(ny - 1, 1), ry, 256), F32),
        pltpu.VMEM((ry, 256), F32),
        pltpu.VMEM((slots, ry, 256), F32),
    ]
    dma = pltpu.SemaphoreType.DMA
    factor, core = pl.pallas_call(
        functools.partial(kernel, nv, nz, ny),
        out_shape=(
            jax.ShapeDtypeStruct((500, 64), F32),
            jax.ShapeDtypeStruct((16 * nv * 8, 128), F32),
        ),
        in_specs=[
            pl.BlockSpec(memory_space=pltpu.SMEM),
            pl.BlockSpec(memory_space=pl.ANY),
            pl.BlockSpec(memory_space=pltpu.VMEM),
        ],
        out_specs=(pl.BlockSpec(memory_space=pltpu.VMEM), pl.BlockSpec(memory_space=pltpu.VMEM)),
        scratch_shapes=[
            pltpu.VMEM((nv, 2) + block, F32),
            pltpu.VMEM((nv, 2) + block, F32),
            pltpu.VMEM((nv,) + block, F32),
            pltpu.VMEM((nv,) + block, F32),
            pltpu.VMEM((nv, 512, 512), BF16),
            pltpu.VMEM((nv, 512, 512), BF16),
            pltpu.VMEM((256, 512), BF16),
            pltpu.VMEM((256, 512), BF16),
            pltpu.VMEM((128, 256), F32),
            pltpu.VMEM((128, 256), F32),
            *reduce_bufs(2),
            *reduce_bufs(4),
            pltpu.VMEM((2, 256, 256), F32),
            pltpu.VMEM((256, 256), F32),
            pltpu.VMEM((768, 256), BF16),
            pltpu.VMEM((768, 256), BF16),
            pltpu.VMEM((64, 512), F32),
            pltpu.VMEM((64, 512), BF16),
            pltpu.VMEM((64, 512), BF16),
            pltpu.VMEM((nv, 16, 512), F32),
            pltpu.VMEM((nv, 16, 512), F32),
            dma((nv, 2)),
            dma((2, nv)),
            dma((2, nv)),
            dma((2, nv)),
            dma((2, 5, 3)),
            dma((2, 5, 3)),
            dma((2, 4)),
            dma((2, nv)),
        ],
        compiler_params=pltpu.CompilerParams(
            collective_id=0, has_side_effects=True, vmem_limit_bytes=60 * 1024 * 1024
        ),
        name="tucker",
    )(var_scale, x, start_basis)
    return factor, core.reshape(16, nv, 8, 128)


def solution(mesh):
    nz = mesh.shape["gy"]
    ny = mesh.shape["gz"] // 2
    in_specs = (P(None, "gx", "gy", "gz"), P(), P())
    out_specs = (P(), P("gx", None, "gy", "gz"))
    return jax.shard_map(
        functools.partial(per_device, nz, ny), mesh=mesh, in_specs=in_specs, out_specs=out_specs, check_vma=False
    )
```

```python
import functools

import jax
import jax.numpy as jnp
from jax import lax
from jax.experimental import pallas as pl
from jax.experimental.pallas import tpu as pltpu
from jax.sharding import PartitionSpec as P

ITERS = 3
MESH = pl.DeviceIdType.MESH
NN = (((1,), (0,)), ((), ()))
NT = (((1,), (1,)), ((), ()))
F32 = jnp.float32
BF16 = jnp.bfloat16
HI = lax.Precision.HIGHEST


def split(x):
    hi = x.astype(BF16)
    return hi, (x - hi.astype(F32)).astype(BF16)


def dot(a, b, dims):
    return lax.dot_general(a, b, dims, preferred_element_type=F32)


def dot3(ah, al, bh, bl, dims):
    return dot(ah, bh, dims) + (dot(ah, bl, dims) + dot(al, bh, dims))


def column(block, j):
    return block.reshape(512, 128)[pl.ds(j, 128, stride=4), :]


def eliminate(m):
    tiles = [m[8 * t : 8 * t + 8, :] for t in range(8)]
    sub = lax.broadcasted_iota(jnp.int32, (8, 128), 0)
    for q in range(8):
        cols = [
            {t: jnp.broadcast_to(tiles[t][:, 8 * q + k : 8 * q + k + 1], (8, 128)) for t in range(q, 8)}
            for k in range(8)
        ]
        pivots = jnp.ones((8, 128), F32)
        for k in range(8):
            p = jnp.broadcast_to(cols[k][q][k : k + 1, :], (8, 128))
            rp = 1.0 / p
            row = jnp.broadcast_to(tiles[q][k : k + 1, :], (8, 128))
            across = {l: jnp.broadcast_to(cols[l][q][k : k + 1, :], (8, 128)) for l in range(k + 1, 8)}
            for t in range(q, 8):
                f = cols[k][t] * rp
                if t == q:
                    f = jnp.where(sub > k, f, 0.0)
                tiles[t] = tiles[t] - f * row
                for l in range(k + 1, 8):
                    cols[l][t] = cols[l][t] - f * across[l]
            pivots = jnp.where(sub == k, p, pivots)
        r = lax.rsqrt(pivots)
        r = r * (1.5 - 0.5 * (pivots * r) * r)
        tiles[q] = tiles[q] * r
    return jnp.concatenate(tiles, axis=0)


def kernel(
    nv, nz, ny, scale_ref, x_ref, start_ref,
    factor_ref, core_ref,
    xo, xd, xx, xf, Xh, Xl, Yh, Yl,
    acc_own, acc_ab,
    pb_o, b2_o, xb_o, pb_a, b2_a, xb_a,
    gd, gx_, gh, gl, bt, fh, fl, psend, precv,
    s_loc, s_d2d, s_x, s_fw, s_ro, s_ra, s_g, s_c,
):
    me = lax.axis_index("gx")
    z = lax.axis_index("gy")
    hy = lax.axis_index("gz")
    h = me // 2
    c = lax.rem(me, 2)
    o = 1 - h
    xh = hy // ny
    y = lax.rem(hy, ny)
    ry = 128 // (nz * ny)

    def dev(gx=me, gy=z, xhi=xh, yy=y):
        return {"gx": gx, "gy": gy, "gz": xhi * ny + yy}

    mate = dev(gx=2 * h + (1 - c))
    across = dev(gx=2 * o + c)
    np_ = nz * ny - 1
    spot = z * ny + y
    plane = []
    for dz in range(nz):
        for dy in range(ny):
            if dz or dy:
                tz, ty = lax.rem(z + dz, nz), lax.rem(y + dy, ny)
                plane.append((dz * ny + dy, tz * ny + ty, dev(gy=tz, yy=ty)))
    x_hi = dev(xhi=1 - xh)
    x_all = [x_hi, across, dev(gx=2 * o + c, xhi=1 - xh)]

    def rcopy(src, dst, sems, at, to):
        return pltpu.make_async_remote_copy(
            src_ref=src, dst_ref=dst, send_sem=sems.at[(0,) + at], recv_sem=sems.at[(1,) + at],
            device_id=to, device_id_type=MESH,
        )

    def local(v, half):
        return pltpu.make_async_copy(x_ref.at[v, :, half], xo.at[v, half, 0:125], s_loc.at[v, half])

    def c_d2d(v):
        return rcopy(xo.at[v, :, 0:125], xd.at[v, :, 0:125], s_d2d, (v,), mate)

    def c_x(v):
        return rcopy(xo.at[v, o, 0:125], xx.at[v, 0:125], s_x, (v,), across)

    def c_fw(v):
        return rcopy(xx.at[v, 0:125], xf.at[v, 0:125], s_fw, (v,), mate)

    for v in range(nv):
        local(v, o).start()
        local(v, h).start()

    barrier = pltpu.get_barrier_semaphore()
    greet = [mate] + [d for _, _, d in plane] + x_all
    for d in greet:
        pl.semaphore_signal(barrier, inc=1, device_id=d, device_id_type=MESH)
    zero = jnp.zeros((3, 4, 128), F32)
    for v in range(nv):
        for half in range(2):
            xo[v, half, 125:128] = zero
            xd[v, half, 125:128] = zero
        xx[v, 125:128] = zero
        xf[v, 125:128] = zero
    pl.semaphore_wait(barrier, len(greet))

    ahead = min(4, nv)

    @pl.loop(0, nv)
    def _(v):
        local(v, o).wait()

        @pl.when(v < ahead)
        def _():
            c_x(v).start()

        local(v, h).wait()
        c_d2d(v).start()

    acc_own[...] = jnp.zeros_like(acc_own)
    acc_ab[...] = jnp.zeros_like(acc_ab)
    bt[...] = jnp.zeros_like(bt)
    for g in range(4):
        bt[:, 128 * g : 128 * g + 125] = start_ref[:, 125 * g : 125 * g + 125]

    def convert(block, s, dh, dl):
        for j in range(4):
            hi, lo = split(column(block, j) * s)
            dh[:, 128 * j : 128 * j + 128] = hi
            dl[:, 128 * j : 128 * j + 128] = lo

    def rows(g, n=128):
        return pl.ds(pl.multiple_of(g * 128, 128), n)

    @pl.loop(0, nv)
    def _(v):
        s = scale_ref[v]
        convert(xo.at[v, h], s, Xh.at[v, rows(me)], Xl.at[v, rows(me)])
        convert(xo.at[v, o], s, Yh.at[rows(c)], Yl.at[rows(c)])
        c_d2d(v).wait_recv()
        m2 = 2 * h + (1 - c)
        convert(xd.at[v, h], s, Xh.at[v, rows(m2)], Xl.at[v, rows(m2)])
        convert(xd.at[v, o], s, Yh.at[rows(1 - c)], Yl.at[rows(1 - c)])
        chip = pl.ds(pl.multiple_of(h * 256, 256), 256)
        acc_own[...] += dot3(
            Xh[v, rows(me), :], Xl[v, rows(me), :], Xh[v, chip, :], Xl[v, chip, :], NT
        ) + dot3(Yh[rows(c), :], Yl[rows(c), :], Yh[...], Yl[...], NT)

    class Reduce:
        def __init__(self, acc, pb, b2, xb, out, sems, partners, slot, slots):
            self.acc, self.pb, self.b2, self.xb = acc, pb, b2, xb
            self.out, self.sems, self.partners, self.slot, self.slots = out, sems, partners, slot, slots

        def piece(self, start):
            return pl.ds(pl.multiple_of(start, ry), ry)

        def rs(self, k):
            _, to, d = plane[k]
            return rcopy(self.acc.at[self.piece(to * ry)], self.pb.at[k], self.sems, (k,), d)

        def xc(self, k):
            return rcopy(self.b2, self.xb.at[self.slot], self.sems, (2 * np_ + k,), self.partners[k])

        def ag(self, k):
            here = self.out.at[self.piece(c * 128 + spot * ry)]
            return rcopy(here, here, self.sems, (np_ + k,), plane[k][2])

        def s0(self):
            for k in range(np_):
                self.rs(k).start()

        def s1(self):
            for k in range(np_):
                self.rs(k).wait_recv()
            t = self.acc[self.piece(spot * ry), :]
            for k in range(np_):
                t = t + self.pb[k]
            self.b2[...] = t
            for k in range(len(self.partners)):
                self.xc(k).start()
            self.xb[self.slot] = t

        def s2(self):
            for k in range(len(self.partners)):
                self.xc(k).wait_recv()
            t = self.xb[0]
            for k in range(1, self.slots):
                t = t + self.xb[k]
            self.out[self.piece(c * 128 + spot * ry), :] = t
            for k in range(np_):
                self.ag(k).start()

        def s3(self):
            for k in range(np_):
                self.ag(k).wait_recv()

        def finish(self):
            for k in range(np_):
                self.rs(k).wait_send()
                self.ag(k).wait_send()
            for k in range(len(self.partners)):
                self.xc(k).wait_send()

    own = Reduce(acc_own, pb_o, b2_o, xb_o, gd.at[h], s_ro, [x_hi], xh, 2)
    ab = Reduce(acc_ab, pb_a, b2_a, xb_a, gx_, s_ra, x_all, xh * 2 + h, 4)

    mine = pl.ds(pl.multiple_of(c * 128, 128), 128)
    g_d2d = rcopy(gd.at[h, mine], gd.at[h, mine], s_g, (0,), mate)
    g_x = rcopy(gd.at[h, mine], gd.at[h, mine], s_g, (1,), across)
    g_got = rcopy(gd.at[o, mine], gd.at[o, mine], s_g, (1,), across)
    g_fw = rcopy(gd.at[o, mine], gd.at[o, mine], s_g, (2,), mate)
    g_ab = rcopy(gx_.at[mine], gx_.at[mine], s_g, (3,), mate)

    def own_done():
        own.s3()
        g_x.start()
        g_d2d.start()

    own.s0()
    steps = {1: own.s1, 8: own.s2, 10: own_done}

    @pl.loop(0, nv)
    def _(v):
        s = scale_ref[v]
        c_x(v).wait_recv()

        @pl.when(v + ahead < nv)
        def _():
            c_x(v + ahead).start()

        c_fw(v).start()
        g2 = 2 * o + c
        convert(xx.at[v], s, Xh.at[v, rows(g2)], Xl.at[v, rows(g2)])
        for k, f in steps.items():
            pl.when(v == k * nv // 11)(f)
        c_fw(v).wait_recv()
        g3 = 2 * o + (1 - c)
        convert(xf.at[v], s, Xh.at[v, rows(g3)], Xl.at[v, rows(g3)])
        acc_ab[...] += dot3(
            Xh[v, rows(c), :], Xl[v, rows(c), :], Xh[v, 256:512, :], Xl[v, 256:512, :], NT
        )

    ab.s0()
    ab.s1()
    g_got.wait_recv()
    g_fw.start()
    ab.s2()
    g_d2d.wait_recv()
    g_fw.wait_recv()
    gh[0:256], gl[0:256] = split(gd[0])
    gh[256:512], gl[256:512] = split(gd[1])
    ab.s3()
    g_ab.start()
    g_ab.wait_recv()
    gh[512:768], gl[512:768] = split(gx_[...])

    pad = jnp.zeros((64, 512), F32)
    rr = lax.broadcasted_iota(jnp.int32, (64, 128), 0)
    cc = lax.broadcasted_iota(jnp.int32, (64, 128), 1)
    eye = jnp.where(cc == rr + 64, 1.0, 0.0).astype(F32)

    @pl.loop(0, ITERS)
    def _(step):
        bh, bl = split(bt[...])
        d0 = gh[0:256, :], gl[0:256, :]
        d1 = gh[256:512, :], gl[256:512, :]
        ax = gh[512:768, :], gl[512:768, :]
        ba = bh[:, 0:256], bl[:, 0:256]
        bb = bh[:, 256:512], bl[:, 256:512]
        left = dot3(*ba, *d0, NN) + dot3(*bb, *ax, NT)
        right = dot3(*ba, *ax, NN) + dot3(*bb, *d1, NN)
        block = jnp.concatenate([left, right], axis=1)
        small = lax.dot_general(
            block, jnp.concatenate([block, pad], axis=0), NT, precision=HI, preferred_element_type=F32
        )
        w = eliminate(small + eye)
        w = jnp.where(cc >= 64, w, 0.0)
        bt[...] = lax.dot_general(
            w, jnp.concatenate([pad, block], axis=0), NN, precision=HI, preferred_element_type=F32
        )

    hi, lo = split(bt[...])
    fh[...] = hi
    fl[...] = lo

    def ranks(g):
        return pl.ds(pl.multiple_of(g * 16, 16), 16)

    def c_core(v):
        return rcopy(psend.at[v], precv.at[v], s_c, (v,), across)

    ours, theirs = ranks(me), ranks(2 * o + c)

    @pl.loop(0, nv)
    def _(v):
        ah = jnp.concatenate([fh[theirs, :], fh[ours, :]], axis=0)
        al = jnp.concatenate([fl[theirs, :], fl[ours, :]], axis=0)
        res = dot3(ah, al, Xh[v], Xl[v], NN)
        psend[v] = res[0:16]
        c_core(v).start()
        for j in range(4):
            core_ref[pl.ds(v * 8 + 4 * h + j, 16, stride=8 * nv), :] = res[16:32, 128 * j : 128 * j + 128]

    for g in range(4):
        factor_ref[:, 125 * g : 125 * g + 125] = bt[:, 128 * g : 128 * g + 125]

    @pl.loop(0, nv)
    def _(v):
        c_core(v).wait_recv()
        got = precv[v]
        for j in range(4):
            core_ref[pl.ds(v * 8 + 4 * o + j, 16, stride=8 * nv), :] = got[:, 128 * j : 128 * j + 128]

    @pl.loop(0, nv)
    def _(v):
        c_x(v).wait_send()
        c_d2d(v).wait_send()
        c_fw(v).wait_send()
        c_core(v).wait_send()

    own.finish()
    ab.finish()
    for g in (g_d2d, g_x, g_fw, g_ab):
        g.wait_send()


def per_device(nz, ny, fields, var_scale, start_basis):
    nv = fields.shape[0]
    x = fields.reshape(nv, 125, 2, 4, 128)
    ry = 128 // (nz * ny)
    np_ = nz * ny - 1
    block = (128, 4, 128)
    reduce_bufs = lambda slots: [
        pltpu.VMEM((np_, ry, 256), F32),
        pltpu.VMEM((ry, 256), F32),
        pltpu.VMEM((slots, ry, 256), F32),
    ]
    dma = pltpu.SemaphoreType.DMA
    factor, core = pl.pallas_call(
        functools.partial(kernel, nv, nz, ny),
        out_shape=(
            jax.ShapeDtypeStruct((64, 500), F32),
            jax.ShapeDtypeStruct((16 * nv * 8, 128), F32),
        ),
        in_specs=[
            pl.BlockSpec(memory_space=pltpu.SMEM),
            pl.BlockSpec(memory_space=pl.ANY),
            pl.BlockSpec(memory_space=pltpu.VMEM),
        ],
        out_specs=(pl.BlockSpec(memory_space=pltpu.VMEM), pl.BlockSpec(memory_space=pltpu.VMEM)),
        scratch_shapes=[
            pltpu.VMEM((nv, 2) + block, F32),
            pltpu.VMEM((nv, 2) + block, F32),
            pltpu.VMEM((nv,) + block, F32),
            pltpu.VMEM((nv,) + block, F32),
            pltpu.VMEM((nv, 512, 512), BF16),
            pltpu.VMEM((nv, 512, 512), BF16),
            pltpu.VMEM((256, 512), BF16),
            pltpu.VMEM((256, 512), BF16),
            pltpu.VMEM((128, 256), F32),
            pltpu.VMEM((128, 256), F32),
            *reduce_bufs(2),
            *reduce_bufs(4),
            pltpu.VMEM((2, 256, 256), F32),
            pltpu.VMEM((256, 256), F32),
            pltpu.VMEM((768, 256), BF16),
            pltpu.VMEM((768, 256), BF16),
            pltpu.VMEM((64, 512), F32),
            pltpu.VMEM((64, 512), BF16),
            pltpu.VMEM((64, 512), BF16),
            pltpu.VMEM((nv, 16, 512), F32),
            pltpu.VMEM((nv, 16, 512), F32),
            dma((nv, 2)),
            dma((2, nv)),
            dma((2, nv)),
            dma((2, nv)),
            dma((2, 2 * np_ + 3)),
            dma((2, 2 * np_ + 3)),
            dma((2, 4)),
            dma((2, nv)),
        ],
        compiler_params=pltpu.CompilerParams(
            collective_id=0, has_side_effects=True, vmem_limit_bytes=60 * 1024 * 1024
        ),
        name="tucker",
    )(var_scale, x, start_basis.T)
    return factor.T, core.reshape(16, nv, 8, 128)


def solution(mesh):
    nz = mesh.shape["gy"]
    ny = mesh.shape["gz"] // 2
    in_specs = (P(None, "gx", "gy", "gz"), P(), P())
    out_specs = (P(), P("gx", None, "gy", "gz"))
    return jax.shard_map(
        functools.partial(per_device, nz, ny), mesh=mesh, in_specs=in_specs, out_specs=out_specs, check_vma=False
    )
```

```python
import functools

import jax
import jax.numpy as jnp
from jax import lax
from jax.experimental import pallas as pl
from jax.experimental.pallas import tpu as pltpu
from jax.sharding import PartitionSpec as P

ITERS = 3
MESH = pl.DeviceIdType.MESH
NN = (((1,), (0,)), ((), ()))
NT = (((1,), (1,)), ((), ()))
F32 = jnp.float32
BF16 = jnp.bfloat16
HI = lax.Precision.HIGHEST


def split(x):
    hi = x.astype(BF16)
    return hi, (x - hi.astype(F32)).astype(BF16)


def dot(a, b, dims):
    return lax.dot_general(a, b, dims, preferred_element_type=F32)


def dot3(ah, al, bh, bl, dims):
    return dot(ah, bh, dims) + (dot(ah, bl, dims) + dot(al, bh, dims))


def column(block, j):
    return block.reshape(512, 128)[pl.ds(j, 128, stride=4), :]


def eliminate(m):
    tiles = [m[8 * t : 8 * t + 8, :] for t in range(8)]
    sub = lax.broadcasted_iota(jnp.int32, (8, 128), 0)

    def spread_row(tile, k):
        return jnp.broadcast_to(tile[k : k + 1, :], (8, 128))

    for first in range(0, 64, 16):
        top = first // 8
        cols = [
            {t: jnp.broadcast_to(tiles[t][:, first + k : first + k + 1], (8, 128)) for t in range(top, 8)}
            for k in range(16)
        ]
        for k in range(16):
            q, r = top + k // 8, k % 8
            if r == 0:
                pivots = jnp.ones((8, 128), F32)
            p = spread_row(cols[k][q], r)
            rp = 1.0 / p
            row = spread_row(tiles[q], r)
            across = {l: spread_row(cols[l][q], r) for l in range(k + 1, 16)}
            for t in range(q, 8):
                f = cols[k][t] * rp
                if t == q:
                    f = jnp.where(sub > r, f, 0.0)
                tiles[t] = tiles[t] - f * row
                for l in range(k + 1, 16):
                    cols[l][t] = cols[l][t] - f * across[l]
            pivots = jnp.where(sub == r, p, pivots)
            if r == 7:
                y = lax.rsqrt(pivots)
                tiles[q] = tiles[q] * (y * (1.5 - 0.5 * (pivots * y) * y))
    return jnp.concatenate(tiles, axis=0)


def kernel(
    nv, ne, nz, ny, scale_ref, x_ref, start_ref,
    factor_ref, core_ref,
    xo, xd, xx, xf, xe, xg, Xh, Xl, Yh, Yl,
    acc_own, acc_ab,
    pb_o, b2_o, xb_o, pb_a, b2_a, xb_a,
    gd, gk, gm, gh, gl, bt, fh, fl, psend, precv,
    s_loc, s_d2d, s_x, s_fw, s_e, s_ef, s_ro, s_ra, s_g, s_c,
):
    me = lax.axis_index("gx")
    z = lax.axis_index("gy")
    hy = lax.axis_index("gz")
    h = me // 2
    c = lax.rem(me, 2)
    o = 1 - h
    xh = hy // ny
    y = lax.rem(hy, ny)
    ry = 128 // (nz * ny)

    def dev(gx=me, gy=z, xhi=xh, yy=y):
        return {"gx": gx, "gy": gy, "gz": xhi * ny + yy}

    mate = dev(gx=2 * h + (1 - c))
    across = dev(gx=2 * o + c)
    np_ = nz * ny - 1
    spot = z * ny + y
    plane = []
    for dz in range(nz):
        for dy in range(ny):
            if dz or dy:
                tz, ty = lax.rem(z + dz, nz), lax.rem(y + dy, ny)
                plane.append((dz * ny + dy, tz * ny + ty, dev(gy=tz, yy=ty)))
    x_hi = dev(xhi=1 - xh)
    x_all = [x_hi, across, dev(gx=2 * o + c, xhi=1 - xh)]
    x_cross = [dev(gx=2 * o + (1 - c)), dev(gx=2 * o + (1 - c), xhi=1 - xh)]

    def rcopy(src, dst, sems, at, to):
        return pltpu.make_async_remote_copy(
            src_ref=src, dst_ref=dst, send_sem=sems.at[(0,) + at], recv_sem=sems.at[(1,) + at],
            device_id=to, device_id_type=MESH,
        )

    def local(v, half):
        return pltpu.make_async_copy(x_ref.at[v, :, half], xo.at[v, half, 0:125], s_loc.at[v, half])

    def c_d2d(v):
        return rcopy(xo.at[v, :, 0:125], xd.at[v, :, 0:125], s_d2d, (v,), mate)

    def c_x(v):
        return rcopy(xo.at[v, o, 0:125], xx.at[v, 0:125], s_x, (v,), across)

    def c_fw(v):
        return rcopy(xx.at[v, 0:125], xf.at[v, 0:125], s_fw, (v,), mate)

    def c_e(v):
        return rcopy(xo.at[v, h, 0:125], xe.at[v, 0:125], s_e, (v,), across)

    def c_ef(v):
        return rcopy(xe.at[v, 0:125], xg.at[v, 0:125], s_ef, (v,), mate)

    for v in range(nv):
        local(v, o).start()
        local(v, h).start()

    barrier = pltpu.get_barrier_semaphore()
    greet = [mate] + [d for _, _, d in plane] + x_all + x_cross
    for d in greet:
        pl.semaphore_signal(barrier, inc=1, device_id=d, device_id_type=MESH)
    zero = jnp.zeros((3, 4, 128), F32)
    for v in range(nv):
        for half in range(2):
            xo[v, half, 125:128] = zero
            xd[v, half, 125:128] = zero
        xx[v, 125:128] = zero
        xf[v, 125:128] = zero
    for v in range(ne):
        xe[v, 125:128] = zero
        xg[v, 125:128] = zero
    pl.semaphore_wait(barrier, len(greet))

    ahead = min(4, nv)

    @pl.loop(0, nv)
    def _(v):
        local(v, o).wait()

        @pl.when(v < ahead)
        def _():
            c_x(v).start()

        local(v, h).wait()
        c_d2d(v).start()

    acc_own[...] = jnp.zeros_like(acc_own)
    acc_ab[...] = jnp.zeros_like(acc_ab)
    bt[...] = jnp.zeros_like(bt)
    for g in range(4):
        bt[:, 128 * g : 128 * g + 125] = start_ref[:, 125 * g : 125 * g + 125]

    def convert(block, s, dh, dl):
        for j in range(4):
            hi, lo = split(column(block, j) * s)
            dh[:, 128 * j : 128 * j + 128] = hi
            dl[:, 128 * j : 128 * j + 128] = lo

    def rows(g, n=128):
        return pl.ds(pl.multiple_of(g * 128, 128), n)

    @pl.loop(0, nv)
    def _(v):
        s = scale_ref[v]
        w = jnp.minimum(v, ne)
        convert(xo.at[v, h], s, Xh.at[v, rows(me)], Xl.at[v, rows(me)])
        convert(xo.at[v, o], s, Yh.at[w, rows(me)], Yl.at[w, rows(me)])
        c_d2d(v).wait_recv()
        m2 = 2 * h + (1 - c)
        convert(xd.at[v, h], s, Xh.at[v, rows(m2)], Xl.at[v, rows(m2)])
        convert(xd.at[v, o], s, Yh.at[w, rows(m2)], Yl.at[w, rows(m2)])
        chip = pl.ds(pl.multiple_of(h * 256, 256), 256)
        acc_own[...] += dot3(
            Xh[v, rows(me), :], Xl[v, rows(me), :], Xh[v, chip, :], Xl[v, chip, :], NT
        ) + dot3(Yh[w, rows(me), :], Yl[w, rows(me), :], Yh[w, chip, :], Yl[w, chip, :], NT)

    def piece(base, p):
        return pl.ds(pl.multiple_of(base + p * ry, ry), ry)

    my_rows = piece(c * 128, spot)
    mine = pl.ds(pl.multiple_of(c * 128, 128), 128)

    def o_rs(k):
        _, to, d = plane[k]
        return rcopy(acc_own.at[piece(0, to)], pb_o.at[k], s_ro, (k,), d)

    def o_x(k):
        return rcopy(b2_o, xb_o.at[xh, h], s_ro, (2 * np_ + k,), x_all[k])

    def o_ag(k):
        return rcopy(gd.at[:, my_rows], gd.at[:, my_rows], s_ro, (np_ + k,), plane[k][2])

    g_own = rcopy(gd.at[:, mine], gd.at[:, mine], s_g, (0,), mate)

    def own_1():
        for k in range(np_):
            o_rs(k).wait_recv()
        t = acc_own[piece(0, spot), :]
        for k in range(np_):
            t = t + pb_o[k]
        b2_o[...] = t
        for k in range(3):
            o_x(k).start()
        xb_o[xh, h] = t

    def own_2():
        for k in range(3):
            o_x(k).wait_recv()
        for side in range(2):
            gd[side, my_rows, :] = xb_o[0, side] + xb_o[1, side]
        for k in range(np_):
            o_ag(k).start()

    def own_3():
        for k in range(np_):
            o_ag(k).wait_recv()
        g_own.start()

    def a_rs(k):
        _, to, d = plane[k]
        return rcopy(acc_ab.at[:, piece(0, to)], pb_a.at[k], s_ra, (k,), d)

    def a_x(k):
        at = (2 * np_ + k,)
        if k == 0:
            return rcopy(b2_a, xb_a.at[xh, h], s_ra, at, x_hi)
        if k < 3:
            return rcopy(b2_a.at[c], xb_a.at[xh, h, c], s_ra, at, x_all[k])
        return rcopy(b2_a.at[1 - c], xb_a.at[xh, h, c], s_ra, at, x_cross[k - 3])

    def a_ag(k):
        here = gk.at[:, piece(0, spot)]
        return rcopy(here, here, s_ra, (np_ + k,), plane[k][2])

    g_ab = rcopy(gk, gm, s_g, (1,), mate)

    for k in range(np_):
        o_rs(k).start()
    steps = {1: own_1, 7: own_2, 9: own_3}
    g2 = 2 * o + c
    g3 = 2 * o + (1 - c)

    def late(v):
        c_fw(v).wait_recv()
        convert(xf.at[v], scale_ref[v], Xh.at[v, rows(g3)], Xl.at[v, rows(g3)])

    @pl.loop(0, nv)
    def _(v):
        c_x(v).wait_recv()

        @pl.when(v + ahead < nv)
        def _():
            c_x(v + ahead).start()

        c_fw(v).start()
        convert(xx.at[v], scale_ref[v], Xh.at[v, rows(g2)], Xl.at[v, rows(g2)])
        for k, f in steps.items():
            pl.when(v == k * nv // 11)(f)
        for k in range(2):
            left = rows(g2 + (1 - h) * (2 * h + k - g2))
            right = rows(g2 + h * (2 * h + k - g2))
            acc_ab[k] += dot3(Xh[v, left, :], Xl[v, left, :], Xh[v, right, :], Xl[v, right, :], NT)

        @pl.when((v > 0) & (v < nv - 1))
        def _():
            late(v - 1)

    for k in range(np_):
        a_rs(k).start()
    c_e(0).start()
    late(nv - 2)
    late(nv - 1)
    g_own.wait_recv()
    gh[0:256], gl[0:256] = split(gd[0])
    gh[256:512], gl[256:512] = split(gd[1])
    for k in range(np_):
        a_rs(k).wait_recv()
    t = acc_ab[:, piece(0, spot), :]
    for k in range(np_):
        t = t + pb_a[k]
    b2_a[...] = t
    for k in range(5):
        a_x(k).start()
    xb_a[xh, h] = t
    for v in range(1, ne):
        c_e(v).start()
    for k in range(3):
        a_x(k).wait_recv()
    for k in range(3, 5):
        rcopy(b2_a.at[1 - c], xb_a.at[xh, o, 1 - c], s_ra, (2 * np_ + k,), x_cross[k - 3]).wait_recv()
    gk[:, piece(0, spot), :] = (xb_a[0, 0] + xb_a[0, 1]) + (xb_a[1, 0] + xb_a[1, 1])
    for k in range(np_):
        a_ag(k).start()
    c_e(0).wait_recv()
    c_ef(0).start()
    for k in range(np_):
        a_ag(k).wait_recv()
    g_ab.start()

    def spread(ref, core):
        for k in range(2):
            hi, lo = split(ref[k])
            at = pl.ds(pl.multiple_of(512 + 128 * (core + (1 - h) * (k - core)), 128), 128)
            to = pl.ds(pl.multiple_of(128 * (core + h * (k - core)), 128), 128)
            gh[at, to] = hi
            gl[at, to] = lo

    spread(gk, c)
    g_ab.wait_recv()
    spread(gm, 1 - c)

    pad = jnp.zeros((64, 512), F32)
    rr = lax.broadcasted_iota(jnp.int32, (64, 128), 0)
    cc = lax.broadcasted_iota(jnp.int32, (64, 128), 1)
    eye = jnp.where(cc == rr + 64, 1.0, 0.0).astype(F32)

    def times_gram(b):
        bh, bl = split(b)
        d0 = gh[0:256, :], gl[0:256, :]
        d1 = gh[256:512, :], gl[256:512, :]
        ax = gh[512:768, :], gl[512:768, :]
        ba = bh[:, 0:256], bl[:, 0:256]
        bb = bh[:, 256:512], bl[:, 256:512]
        left = dot3(*ba, *d0, NN) + dot3(*bb, *ax, NT)
        right = dot3(*ba, *ax, NN) + dot3(*bb, *d1, NN)
        return jnp.concatenate([left, right], axis=1)

    block = times_gram(bt[...])
    for step in range(ITERS):
        small = lax.dot_general(
            block, jnp.concatenate([block, pad], axis=0), NT, precision=HI, preferred_element_type=F32
        )
        after = times_gram(block) if step < ITERS - 1 else block
        w = eliminate(small + eye)
        w = jnp.where(cc >= 64, w, 0.0)
        block = dot3(*split(w), *split(jnp.concatenate([pad, after], axis=0)), NN)
        if 1 <= step < ne:
            c_e(step).wait_recv()
            c_ef(step).start()
    bt[...] = block

    hi, lo = split(bt[...])
    fh[...] = hi
    fl[...] = lo

    def ranks(g):
        return pl.ds(pl.multiple_of(g * 16, 16), 16)

    def c_core(v):
        return rcopy(psend.at[v], precv.at[v], s_c, (v,), across)

    ours, theirs = ranks(me), ranks(2 * o + c)

    def put(v, half, val):
        for j in range(4):
            core_ref[pl.ds(v * 8 + 4 * half + j, 16, stride=8 * nv), :] = val[:, 128 * j : 128 * j + 128]

    @pl.loop(ne, nv)
    def _(v):
        ah = jnp.concatenate([fh[theirs, :], fh[ours, :]], axis=0)
        al = jnp.concatenate([fl[theirs, :], fl[ours, :]], axis=0)
        res = dot3(ah, al, Xh[v], Xl[v], NN)
        psend[v] = res[0:16]
        c_core(v).start()
        put(v, h, res[16:32])

    for g in range(4):
        factor_ref[:, 125 * g : 125 * g + 125] = bt[:, 128 * g : 128 * g + 125]

    for v in range(ITERS, ne):
        c_e(v).wait_recv()
        c_ef(v).start()

    @pl.loop(0, ne)
    def _(v):
        put(v, h, dot3(fh[ours, :], fl[ours, :], Xh[v], Xl[v], NN))
        s = scale_ref[v]
        convert(xe.at[v], s, Yh.at[v, rows(g2)], Yl.at[v, rows(g2)])
        c_ef(v).wait_recv()
        convert(xg.at[v], s, Yh.at[v, rows(g3)], Yl.at[v, rows(g3)])
        put(v, o, dot3(fh[ours, :], fl[ours, :], Yh[v], Yl[v], NN))

    @pl.loop(ne, nv)
    def _(v):
        c_core(v).wait_recv()
        put(v, o, precv[v])

    @pl.loop(0, nv)
    def _(v):
        c_x(v).wait_send()
        c_d2d(v).wait_send()
        c_fw(v).wait_send()

    @pl.loop(ne, nv)
    def _(v):
        c_core(v).wait_send()

    @pl.loop(0, ne)
    def _(v):
        c_e(v).wait_send()
        c_ef(v).wait_send()

    for k in range(np_):
        for f in (o_rs, o_ag, a_rs, a_ag):
            f(k).wait_send()
    for k in range(3):
        o_x(k).wait_send()
    for k in range(5):
        a_x(k).wait_send()
    g_own.wait_send()
    g_ab.wait_send()


def finish(f_ref, c_ref, fo_ref, co_ref, sems):
    copies = [pltpu.make_async_copy(c_ref, co_ref, sems.at[0]), pltpu.make_async_copy(f_ref, fo_ref, sems.at[1])]
    for copy in copies:
        copy.start()
    for copy in copies:
        copy.wait()


def per_device(nz, ny, fields, var_scale, start_basis):
    nv = fields.shape[0]
    x = fields.reshape(nv, 125, 2, 4, 128)
    ry = 128 // (nz * ny)
    np_ = nz * ny - 1
    block = (128, 4, 128)
    ne = min(4, nv - 1)
    dma = pltpu.SemaphoreType.DMA
    factor, core = pl.pallas_call(
        functools.partial(kernel, nv, ne, nz, ny),
        out_shape=(
            jax.ShapeDtypeStruct((64, 500), F32),
            jax.ShapeDtypeStruct((16 * nv * 8, 128), F32),
        ),
        in_specs=[
            pl.BlockSpec(memory_space=pltpu.SMEM),
            pl.BlockSpec(memory_space=pl.ANY),
            pl.BlockSpec(memory_space=pltpu.VMEM),
        ],
        out_specs=(pl.BlockSpec(memory_space=pltpu.VMEM), pl.BlockSpec(memory_space=pltpu.VMEM)),
        scratch_shapes=[
            pltpu.VMEM((nv, 2) + block, F32),
            pltpu.VMEM((nv, 2) + block, F32),
            pltpu.VMEM((nv,) + block, F32),
            pltpu.VMEM((nv,) + block, F32),
            pltpu.VMEM((ne,) + block, F32),
            pltpu.VMEM((ne,) + block, F32),
            pltpu.VMEM((nv, 512, 512), BF16),
            pltpu.VMEM((nv, 512, 512), BF16),
            pltpu.VMEM((ne + 1, 512, 512), BF16),
            pltpu.VMEM((ne + 1, 512, 512), BF16),
            pltpu.VMEM((128, 256), F32),
            pltpu.VMEM((2, 128, 128), F32),
            pltpu.VMEM((np_, ry, 256), F32),
            pltpu.VMEM((ry, 256), F32),
            pltpu.VMEM((2, 2, ry, 256), F32),
            pltpu.VMEM((np_, 2, ry, 128), F32),
            pltpu.VMEM((2, ry, 128), F32),
            pltpu.VMEM((2, 2, 2, ry, 128), F32),
            pltpu.VMEM((2, 256, 256), F32),
            pltpu.VMEM((2, 128, 128), F32),
            pltpu.VMEM((2, 128, 128), F32),
            pltpu.VMEM((768, 256), BF16),
            pltpu.VMEM((768, 256), BF16),
            pltpu.VMEM((64, 512), F32),
            pltpu.VMEM((64, 512), BF16),
            pltpu.VMEM((64, 512), BF16),
            pltpu.VMEM((nv, 16, 512), F32),
            pltpu.VMEM((nv, 16, 512), F32),
            dma((nv, 2)),
            dma((2, nv)),
            dma((2, nv)),
            dma((2, nv)),
            dma((2, ne)),
            dma((2, ne)),
            dma((2, 2 * np_ + 3)),
            dma((2, 2 * np_ + 5)),
            dma((2, 2)),
            dma((2, nv)),
        ],
        compiler_params=pltpu.CompilerParams(
            collective_id=0, has_side_effects=True, vmem_limit_bytes=60 * 1024 * 1024
        ),
        name="tucker",
    )(var_scale, x, start_basis.T)
    factor, core = pl.pallas_call(
        finish,
        out_shape=(jax.ShapeDtypeStruct((64, 500), F32), jax.ShapeDtypeStruct((16 * nv * 8, 128), F32)),
        in_specs=[pl.BlockSpec(memory_space=pltpu.VMEM)] * 2,
        out_specs=[pl.BlockSpec(memory_space=pl.ANY)] * 2,
        scratch_shapes=[dma((2,))],
        name="finish",
    )(factor, core)
    return factor.T, core.reshape(16, nv, 8, 128)


def solution(mesh):
    nz = mesh.shape["gy"]
    ny = mesh.shape["gz"] // 2
    in_specs = (P(None, "gx", "gy", "gz"), P(), P())
    out_specs = (P(), P("gx", None, "gy", "gz"))
    return jax.shard_map(
        functools.partial(per_device, nz, ny), mesh=mesh, in_specs=in_specs, out_specs=out_specs, check_vma=False
    )
```

```python
import functools

import jax
import jax.numpy as jnp
from jax import lax
from jax.experimental import pallas as pl
from jax.experimental.pallas import tpu as pltpu
from jax.sharding import PartitionSpec as P

ITERS = 3
MESH = pl.DeviceIdType.MESH
NN = (((1,), (0,)), ((), ()))
NT = (((1,), (1,)), ((), ()))
F32 = jnp.float32
BF16 = jnp.bfloat16
HI = lax.Precision.HIGHEST


def split(x):
    hi = x.astype(BF16)
    return hi, (x - hi.astype(F32)).astype(BF16)


def dot(a, b, dims):
    return lax.dot_general(a, b, dims, preferred_element_type=F32)


def dot3(ah, al, bh, bl, dims):
    return dot(ah, bh, dims) + (dot(ah, bl, dims) + dot(al, bh, dims))


def column(block, j):
    return block.reshape(512, 128)[pl.ds(j, 128, stride=4), :]


def eliminate(m):
    tiles = [m[8 * t : 8 * t + 8, :] for t in range(8)]
    sub = lax.broadcasted_iota(jnp.int32, (8, 128), 0)

    def spread_row(tile, k):
        return jnp.broadcast_to(tile[k : k + 1, :], (8, 128))

    for first in range(0, 64, 16):
        top = first // 8
        cols = [
            {t: jnp.broadcast_to(tiles[t][:, first + k : first + k + 1], (8, 128)) for t in range(top, 8)}
            for k in range(16)
        ]
        for k in range(16):
            q, r = top + k // 8, k % 8
            if r == 0:
                pivots = jnp.ones((8, 128), F32)
            p = spread_row(cols[k][q], r)
            rp = 1.0 / p
            row = spread_row(tiles[q], r)
            across = {l: spread_row(cols[l][q], r) for l in range(k + 1, 16)}
            for t in range(q, 8):
                f = cols[k][t] * rp
                if t == q:
                    f = jnp.where(sub > r, f, 0.0)
                tiles[t] = tiles[t] - f * row
                for l in range(k + 1, 16):
                    cols[l][t] = cols[l][t] - f * across[l]
            pivots = jnp.where(sub == r, p, pivots)
            if r == 7:
                y = lax.rsqrt(pivots)
                tiles[q] = tiles[q] * (y * (1.5 - 0.5 * (pivots * y) * y))
    return jnp.concatenate(tiles, axis=0)


def kernel(
    nv, ne, nz, ny, scale_ref, x_ref, start_ref,
    factor_ref, core_ref,
    xo, xd, xx, xf, xe, xg, Xh, Xl, Yh, Yl,
    acc_own, acc_ab,
    pb_o, b2_o, xb_o, pb_a, b2_a, xb_a,
    gd, gk, gm, gh, gl, first, bt, fh, fl, psend, precv,
    s_loc, s_d2d, s_x, s_fw, s_e, s_ef, s_ro, s_ra, s_g, s_c, s_in,
):
    me = lax.axis_index("gx")
    z = lax.axis_index("gy")
    hy = lax.axis_index("gz")
    h = me // 2
    c = lax.rem(me, 2)
    o = 1 - h
    xh = hy // ny
    y = lax.rem(hy, ny)
    ry = 128 // (nz * ny)

    def dev(gx=me, gy=z, xhi=xh, yy=y):
        return {"gx": gx, "gy": gy, "gz": xhi * ny + yy}

    mate = dev(gx=2 * h + (1 - c))
    across = dev(gx=2 * o + c)
    zline = [dev(gy=lax.rem(z + d, nz)) for d in range(1, nz)]
    yline = [dev(yy=lax.rem(y + d, ny)) for d in range(1, ny)]
    np_ = nz * ny - 1
    spot = z * ny + y
    plane = []
    for dz in range(nz):
        for dy in range(ny):
            if dz or dy:
                tz, ty = lax.rem(z + dz, nz), lax.rem(y + dy, ny)
                plane.append((dz * ny + dy, tz * ny + ty, dev(gy=tz, yy=ty)))
    x_hi = dev(xhi=1 - xh)
    x_all = [x_hi, across, dev(gx=2 * o + c, xhi=1 - xh)]
    x_cross = [dev(gx=2 * o + (1 - c)), dev(gx=2 * o + (1 - c), xhi=1 - xh)]

    def rcopy(src, dst, sems, at, to):
        return pltpu.make_async_remote_copy(
            src_ref=src, dst_ref=dst, send_sem=sems.at[(0,) + at], recv_sem=sems.at[(1,) + at],
            device_id=to, device_id_type=MESH,
        )

    def local(v, half):
        return pltpu.make_async_copy(x_ref.at[v, :, half], xo.at[v, half, 0:125], s_loc.at[v, half])

    def c_d2d(v):
        return rcopy(xo.at[v, :, 0:125], xd.at[v, :, 0:125], s_d2d, (v,), mate)

    def c_x(v):
        return rcopy(xo.at[v, o, 0:125], xx.at[v, 0:125], s_x, (v,), across)

    def c_fw(v):
        return rcopy(xx.at[v, 0:125], xf.at[v, 0:125], s_fw, (v,), mate)

    def c_e(v):
        return rcopy(xo.at[v, h, 0:125], xe.at[v, 0:125], s_e, (v,), across)

    def c_ef(v):
        return rcopy(xe.at[v, 0:125], xg.at[v, 0:125], s_ef, (v,), mate)

    for v in range(nv):
        local(v, o).start()
        local(v, h).start()

    barrier = pltpu.get_barrier_semaphore()
    greet = [mate, across, x_cross[0], x_hi] + zline + yline
    for d in greet:
        pl.semaphore_signal(barrier, inc=1, device_id=d, device_id_type=MESH)
    zero = jnp.zeros((3, 4, 128), F32)
    for v in range(nv):
        for half in range(2):
            xo[v, half, 125:128] = zero
            xd[v, half, 125:128] = zero
        xx[v, 125:128] = zero
        xf[v, 125:128] = zero
    for v in range(ne):
        xe[v, 125:128] = zero
        xg[v, 125:128] = zero
    pl.semaphore_wait(barrier, len(greet))
    for d in zline + [x_hi]:
        pl.semaphore_signal(s_in, inc=1, device_id=d, device_id_type=MESH)

    ahead = min(4, nv)

    @pl.loop(0, nv)
    def _(v):
        local(v, o).wait()

        @pl.when(v < ahead)
        def _():
            c_x(v).start()

        local(v, h).wait()
        c_d2d(v).start()

    acc_own[...] = jnp.zeros_like(acc_own)
    acc_ab[...] = jnp.zeros_like(acc_ab)
    bt[...] = jnp.zeros_like(bt)
    for g in range(4):
        bt[:, 128 * g : 128 * g + 125] = start_ref[:, 125 * g : 125 * g + 125]

    def convert(block, s, dh, dl):
        for j in range(4):
            hi, lo = split(column(block, j) * s)
            dh[:, 128 * j : 128 * j + 128] = hi
            dl[:, 128 * j : 128 * j + 128] = lo

    def rows(g, n=128):
        return pl.ds(pl.multiple_of(g * 128, 128), n)

    @pl.loop(0, nv)
    def _(v):
        s = scale_ref[v]
        w = jnp.minimum(v, ne)
        convert(xo.at[v, h], s, Xh.at[v, rows(me)], Xl.at[v, rows(me)])
        convert(xo.at[v, o], s, Yh.at[w, rows(me)], Yl.at[w, rows(me)])
        c_d2d(v).wait_recv()
        m2 = 2 * h + (1 - c)
        convert(xd.at[v, h], s, Xh.at[v, rows(m2)], Xl.at[v, rows(m2)])
        convert(xd.at[v, o], s, Yh.at[w, rows(m2)], Yl.at[w, rows(m2)])
        chip = pl.ds(pl.multiple_of(h * 256, 256), 256)
        acc_own[...] += dot3(
            Xh[v, rows(me), :], Xl[v, rows(me), :], Xh[v, chip, :], Xl[v, chip, :], NT
        ) + dot3(Yh[w, rows(me), :], Yl[w, rows(me), :], Yh[w, chip, :], Yl[w, chip, :], NT)

    def piece(base, p):
        return pl.ds(pl.multiple_of(base + p * ry, ry), ry)

    my_rows = piece(c * 128, spot)
    mine = pl.ds(pl.multiple_of(c * 128, 128), 128)

    def o_rs(k):
        _, to, d = plane[k]
        return rcopy(acc_own.at[piece(0, to)], pb_o.at[k], s_ro, (k,), d)

    def o_x(k):
        return rcopy(b2_o, xb_o.at[xh, h], s_ro, (2 * np_ + k,), x_all[k])

    def o_ag(k):
        return rcopy(gd.at[:, my_rows], gd.at[:, my_rows], s_ro, (np_ + k,), plane[k][2])

    g_own = rcopy(gd.at[:, mine], gd.at[:, mine], s_g, (0,), mate)

    def own_1():
        for k in range(np_):
            o_rs(k).wait_recv()
        t = acc_own[piece(0, spot), :]
        for k in range(np_):
            t = t + pb_o[k]
        b2_o[...] = t
        for k in range(3):
            o_x(k).start()
        xb_o[xh, h] = t

    def own_2():
        for k in range(3):
            o_x(k).wait_recv()
        for side in range(2):
            gd[side, my_rows, :] = xb_o[0, side] + xb_o[1, side]
        for k in range(np_):
            o_ag(k).start()

    def own_3():
        for k in range(np_):
            o_ag(k).wait_recv()
        g_own.start()

    def a_rs(k):
        _, to, d = plane[k]
        return rcopy(acc_ab.at[:, piece(0, to)], pb_a.at[k], s_ra, (k,), d)

    def a_x(k):
        at = (2 * np_ + k,)
        if k == 0:
            return rcopy(b2_a, xb_a.at[xh, h], s_ra, at, x_hi)
        if k < 3:
            return rcopy(b2_a.at[c], xb_a.at[xh, h, c], s_ra, at, x_all[k])
        return rcopy(b2_a.at[1 - c], xb_a.at[xh, h, c], s_ra, at, x_cross[k - 3])

    def a_ag(k):
        here = gk.at[:, piece(0, spot)]
        return rcopy(here, here, s_ra, (np_ + k,), plane[k][2])

    g_ab = rcopy(gk, gm, s_g, (1,), mate)

    pl.semaphore_wait(s_in, len(zline) + 1)
    for k in range(np_):
        o_rs(k).start()
    steps = {1: own_1, 7: own_2, 9: own_3}
    g2 = 2 * o + c
    g3 = 2 * o + (1 - c)

    def late(v):
        c_fw(v).wait_recv()
        convert(xf.at[v], scale_ref[v], Xh.at[v, rows(g3)], Xl.at[v, rows(g3)])

    @pl.loop(0, nv)
    def _(v):
        c_x(v).wait_recv()

        @pl.when(v + ahead < nv)
        def _():
            c_x(v + ahead).start()

        c_fw(v).start()
        convert(xx.at[v], scale_ref[v], Xh.at[v, rows(g2)], Xl.at[v, rows(g2)])
        for k, f in steps.items():
            pl.when(v == k * nv // 11)(f)
        for k in range(2):
            left = rows(g2 + (1 - h) * (2 * h + k - g2))
            right = rows(g2 + h * (2 * h + k - g2))
            acc_ab[k] += dot3(Xh[v, left, :], Xl[v, left, :], Xh[v, right, :], Xl[v, right, :], NT)

        @pl.when((v > 0) & (v < nv - 1))
        def _():
            late(v - 1)

    def halves(b):
        bh, bl = split(b)
        return (bh[:, 0:256], bl[:, 0:256]), (bh[:, 256:512], bl[:, 256:512])

    def diagonal(b):
        ba, bb = halves(b)
        left = dot3(*ba, gh[0:256, :], gl[0:256, :], NN)
        right = dot3(*bb, gh[256:512, :], gl[256:512, :], NN)
        return jnp.concatenate([left, right], axis=1)

    def crossing(b):
        ba, bb = halves(b)
        ax = gh[512:768, :], gl[512:768, :]
        return jnp.concatenate([dot3(*bb, *ax, NT), dot3(*ba, *ax, NN)], axis=1)

    for k in range(np_):
        a_rs(k).start()
    c_e(0).start()
    late(nv - 2)
    late(nv - 1)
    g_own.wait_recv()
    gh[0:256], gl[0:256] = split(gd[0])
    gh[256:512], gl[256:512] = split(gd[1])
    first[...] = diagonal(bt[...])
    for k in range(np_):
        a_rs(k).wait_recv()
    t = acc_ab[:, piece(0, spot), :]
    for k in range(np_):
        t = t + pb_a[k]
    b2_a[...] = t
    for k in range(5):
        a_x(k).start()
    xb_a[xh, h] = t
    for v in range(1, ne):
        c_e(v).start()
    for k in range(3):
        a_x(k).wait_recv()
    for k in range(3, 5):
        rcopy(b2_a.at[1 - c], xb_a.at[xh, o, 1 - c], s_ra, (2 * np_ + k,), x_cross[k - 3]).wait_recv()
    gk[:, piece(0, spot), :] = (xb_a[0, 0] + xb_a[0, 1]) + (xb_a[1, 0] + xb_a[1, 1])
    for k in range(np_):
        a_ag(k).start()
    c_e(0).wait_recv()
    c_ef(0).start()
    for k in range(np_):
        a_ag(k).wait_recv()
    g_ab.start()

    def spread(ref, core):
        for k in range(2):
            hi, lo = split(ref[k])
            at = pl.ds(pl.multiple_of(512 + 128 * (core + (1 - h) * (k - core)), 128), 128)
            to = pl.ds(pl.multiple_of(128 * (core + h * (k - core)), 128), 128)
            gh[at, to] = hi
            gl[at, to] = lo

    spread(gk, c)
    g_ab.wait_recv()
    spread(gm, 1 - c)

    pad = jnp.zeros((64, 512), F32)
    rr = lax.broadcasted_iota(jnp.int32, (64, 128), 0)
    cc = lax.broadcasted_iota(jnp.int32, (64, 128), 1)
    eye = jnp.where(cc == rr + 64, 1.0, 0.0).astype(F32)

    block = first[...] + crossing(bt[...])
    for step in range(ITERS):
        small = dot3(*split(block), *split(jnp.concatenate([block, pad], axis=0)), NT)
        after = diagonal(block) + crossing(block) if step < ITERS - 1 else block
        w = eliminate(small + eye)
        w = jnp.where(cc >= 64, w, 0.0)
        block = dot3(*split(w), *split(jnp.concatenate([pad, after], axis=0)), NN)
        if 1 <= step < ne:
            c_e(step).wait_recv()
            c_ef(step).start()
    bt[...] = block

    hi, lo = split(bt[...])
    fh[...] = hi
    fl[...] = lo

    def ranks(g):
        return pl.ds(pl.multiple_of(g * 16, 16), 16)

    def c_core(v):
        return rcopy(psend.at[v], precv.at[v], s_c, (v,), across)

    ours, theirs = ranks(me), ranks(2 * o + c)

    def put(v, half, val):
        for j in range(4):
            core_ref[pl.ds(v * 8 + 4 * half + j, 16, stride=8 * nv), :] = val[:, 128 * j : 128 * j + 128]

    @pl.loop(ne, nv)
    def _(v):
        ah = jnp.concatenate([fh[theirs, :], fh[ours, :]], axis=0)
        al = jnp.concatenate([fl[theirs, :], fl[ours, :]], axis=0)
        res = dot3(ah, al, Xh[v], Xl[v], NN)
        psend[v] = res[0:16]
        c_core(v).start()
        put(v, h, res[16:32])

    for g in range(4):
        factor_ref[:, 125 * g : 125 * g + 125] = bt[:, 128 * g : 128 * g + 125]

    for v in range(ITERS, ne):
        c_e(v).wait_recv()
        c_ef(v).start()

    @pl.loop(0, ne)
    def _(v):
        put(v, h, dot3(fh[ours, :], fl[ours, :], Xh[v], Xl[v], NN))
        s = scale_ref[v]
        convert(xe.at[v], s, Yh.at[v, rows(g2)], Yl.at[v, rows(g2)])
        c_ef(v).wait_recv()
        convert(xg.at[v], s, Yh.at[v, rows(g3)], Yl.at[v, rows(g3)])
        put(v, o, dot3(fh[ours, :], fl[ours, :], Yh[v], Yl[v], NN))

    @pl.loop(ne, nv)
    def _(v):
        c_core(v).wait_recv()
        put(v, o, precv[v])

    @pl.loop(0, nv)
    def _(v):
        c_x(v).wait_send()
        c_d2d(v).wait_send()
        c_fw(v).wait_send()

    @pl.loop(ne, nv)
    def _(v):
        c_core(v).wait_send()

    @pl.loop(0, ne)
    def _(v):
        c_e(v).wait_send()
        c_ef(v).wait_send()

    for k in range(np_):
        for f in (o_rs, o_ag, a_rs, a_ag):
            f(k).wait_send()
    for k in range(3):
        o_x(k).wait_send()
    for k in range(5):
        a_x(k).wait_send()
    g_own.wait_send()
    g_ab.wait_send()


def finish(f_ref, c_ref, fo_ref, co_ref, f_buf, c_buf, sems):
    n = 4
    size = c_ref.shape[0] // n
    parts = [(c_ref.at[pl.ds(i * size, size)], c_buf.at[pl.ds(i * size, size)], co_ref.at[pl.ds(i * size, size)]) for i in range(n)]
    parts.append((f_ref, f_buf, fo_ref))
    reads = [pltpu.make_async_copy(a, b, sems.at[0, i]) for i, (a, b, _) in enumerate(parts)]
    writes = [pltpu.make_async_copy(b, c, sems.at[1, i]) for i, (_, b, c) in enumerate(parts)]
    for copy in reads:
        copy.start()
    for read, write in zip(reads, writes):
        read.wait()
        write.start()
    for copy in writes:
        copy.wait()


def per_device(nz, ny, fields, var_scale, start_basis):
    nv = fields.shape[0]
    x = fields.reshape(nv, 125, 2, 4, 128)
    ry = 128 // (nz * ny)
    np_ = nz * ny - 1
    block = (128, 4, 128)
    ne = min(4, nv - 1)
    dma = pltpu.SemaphoreType.DMA
    factor, core = pl.pallas_call(
        functools.partial(kernel, nv, ne, nz, ny),
        out_shape=(
            jax.ShapeDtypeStruct((64, 500), F32),
            jax.ShapeDtypeStruct((16 * nv * 8, 128), F32),
        ),
        in_specs=[
            pl.BlockSpec(memory_space=pltpu.SMEM),
            pl.BlockSpec(memory_space=pl.ANY),
            pl.BlockSpec(memory_space=pltpu.VMEM),
        ],
        out_specs=(pl.BlockSpec(memory_space=pltpu.VMEM), pl.BlockSpec(memory_space=pltpu.VMEM)),
        scratch_shapes=[
            pltpu.VMEM((nv, 2) + block, F32),
            pltpu.VMEM((nv, 2) + block, F32),
            pltpu.VMEM((nv,) + block, F32),
            pltpu.VMEM((nv,) + block, F32),
            pltpu.VMEM((ne,) + block, F32),
            pltpu.VMEM((ne,) + block, F32),
            pltpu.VMEM((nv, 512, 512), BF16),
            pltpu.VMEM((nv, 512, 512), BF16),
            pltpu.VMEM((ne + 1, 512, 512), BF16),
            pltpu.VMEM((ne + 1, 512, 512), BF16),
            pltpu.VMEM((128, 256), F32),
            pltpu.VMEM((2, 128, 128), F32),
            pltpu.VMEM((np_, ry, 256), F32),
            pltpu.VMEM((ry, 256), F32),
            pltpu.VMEM((2, 2, ry, 256), F32),
            pltpu.VMEM((np_, 2, ry, 128), F32),
            pltpu.VMEM((2, ry, 128), F32),
            pltpu.VMEM((2, 2, 2, ry, 128), F32),
            pltpu.VMEM((2, 256, 256), F32),
            pltpu.VMEM((2, 128, 128), F32),
            pltpu.VMEM((2, 128, 128), F32),
            pltpu.VMEM((768, 256), BF16),
            pltpu.VMEM((768, 256), BF16),
            pltpu.VMEM((64, 512), F32),
            pltpu.VMEM((64, 512), F32),
            pltpu.VMEM((64, 512), BF16),
            pltpu.VMEM((64, 512), BF16),
            pltpu.VMEM((nv, 16, 512), F32),
            pltpu.VMEM((nv, 16, 512), F32),
            dma((nv, 2)),
            dma((2, nv)),
            dma((2, nv)),
            dma((2, nv)),
            dma((2, ne)),
            dma((2, ne)),
            dma((2, 2 * np_ + 3)),
            dma((2, 2 * np_ + 5)),
            dma((2, 2)),
            dma((2, nv)),
            pltpu.SemaphoreType.REGULAR,
        ],
        compiler_params=pltpu.CompilerParams(
            collective_id=0, has_side_effects=True, vmem_limit_bytes=60 * 1024 * 1024
        ),
        name="tucker",
    )(var_scale, x, start_basis.T)
    factor, core = pl.pallas_call(
        finish,
        out_shape=(jax.ShapeDtypeStruct((64, 500), F32), jax.ShapeDtypeStruct((16 * nv * 8, 128), F32)),
        in_specs=[pl.BlockSpec(memory_space=pl.ANY)] * 2,
        out_specs=[pl.BlockSpec(memory_space=pl.ANY)] * 2,
        scratch_shapes=[pltpu.VMEM((64, 500), F32), pltpu.VMEM((16 * nv * 8, 128), F32), dma((2, 5))],
        name="finish",
    )(factor, core)
    return factor.T, core.reshape(16, nv, 8, 128)


def solution(mesh):
    nz = mesh.shape["gy"]
    ny = mesh.shape["gz"] // 2
    in_specs = (P(None, "gx", "gy", "gz"), P(), P())
    out_specs = (P(), P("gx", None, "gy", "gz"))
    return jax.shard_map(
        functools.partial(per_device, nz, ny), mesh=mesh, in_specs=in_specs, out_specs=out_specs, check_vma=False
    )
```
